32 devices in a mesh: frame: 8 (over z, x), row: 4 (over y, core).
Axes of the slice: x: 2, y: 2, z: 4, core: 2. Of those that a mesh axis runs over, the one named last changes fastest.
Arguments:
- clip: bfloat16 [16, 16, 256, 128], P('frame', 'row'), may hold values from -6 to 6
- first_kernel: bfloat16 [3, 3, 3, 128, 128], replicated, may hold values from -0.109375 to 0.109375
- second_kernel: bfloat16 [3, 3, 3, 128, 128], replicated, may hold values from -0.109375 to 0.109375
- cotangent: bfloat16 [16, 16, 256, 128], P('frame', 'row'), may hold values from -6 to 6
Outputs:
- critic_map: bfloat16 [16, 16, 256, 128], P('frame', 'row')
- clip_grad: bfloat16 [16, 16, 256, 128], P('frame', 'row')
- first_grad: float32 [3, 3, 3, 128, 128], replicated
- second_grad: float32 [3, 3, 3, 128, 128], replicated
The draws below stay inside these ranges and needn't reach their ends.
All inputs are finite; a program needn't handle non-finite values.
Results may differ from the reference program's by a relative error of at most 0.012.
Values may be sent and summed in bfloat16 or wider, within the bound.
A program may use at most 64 MiB of HBM per device.

```python
import jax
import jax.numpy as jnp
from jax import lax

CH = 128
WIDTH = 256
FRAMES = 16
ROWS = 16


def level_of(stream_key, extent, shards, low, high):
    loudness = 1.0
    for position, parts in shards:
        draws = jax.random.uniform(jax.random.fold_in(jax.random.fold_in(stream_key, 6), position), (parts,), jnp.float32, low / len(shards), high / len(shards))
        loudness = loudness * jnp.repeat(jnp.exp(draws), extent[position] // parts).reshape((-1,) + (1,) * (len(extent) - 1 - position))
    return loudness


def centred(rng, extent, scale, most, cuts=(), held_as=jnp.bfloat16):
    gain = level_of(rng, extent, cuts, -0.22, 0.18) if cuts else 1.0
    values = jax.random.normal(rng, extent, jnp.float32) * scale * gain
    return jnp.minimum(jnp.maximum(values, -most), most).astype(held_as)


def setup_inputs(seed: int = 0) -> dict:
    key_list = jax.random.split(jax.random.key(seed), 5)
    clip = centred(key_list[0], (FRAMES, ROWS, WIDTH, CH), 1.0, 6.0, ((0, 8), (1, 4)))
    first_kernel = centred(key_list[1], (3, 3, 3, CH, CH), (27 * CH) ** -0.5, 0.109375)
    second_kernel = centred(key_list[2], (3, 3, 3, CH, CH), (27 * CH) ** -0.5, 0.109375)
    cotangent = centred(key_list[3], (FRAMES, ROWS, WIDTH, CH), 1.0, 6.0, ((0, 8), (1, 4)))
    return dict(clip=clip, first_kernel=first_kernel, second_kernel=second_kernel, cotangent=cotangent)


def correlate(padded, kernel):
    result = lax.conv_general_dilated(padded[None], kernel, (1, 1, 1), ((0, 0), (0, 0), (1, 1)), dimension_numbers=('NDHWC', 'DHWIO', 'NDHWC'), preferred_element_type=jnp.float32)
    return result[0]

def silu_slope(value):
    sigma = jax.nn.sigmoid(value)
    return sigma * (1.0 + value * (1.0 - sigma))

def flipped_kernel(kernel):
    return jnp.transpose(kernel[::-1, ::-1, ::-1], (0, 1, 2, 4, 3))

def weight_grad(padded, delta):
    frame_count, row_count, columns, channels = delta.shape
    widened = jnp.pad(padded, ((0, 0), (0, 0), (1, 1), (0, 0)))
    flat_delta = delta.reshape(-1, channels)
    blocks = []
    for frame_off in range(3):
        for row_off in range(3):
            for col_off in range(3):
                window_slab = widened[frame_off:frame_off + frame_count, row_off:row_off + row_count, col_off:col_off + columns]
                blocks.append(lax.dot_general(window_slab.reshape(-1, channels), flat_delta, (((0,), (0,)), ((), ())), preferred_element_type=jnp.float32))
    return jnp.stack(blocks).reshape(3, 3, 3, channels, channels)

def reference(clip, first_kernel, second_kernel, cotangent):
    grad_scale = 1.0 / float(FRAMES * ROWS * WIDTH) ** 0.5
    clip_pad = jnp.pad(clip, ((2, 0), (1, 1), (0, 0), (0, 0)))
    first_pre = correlate(clip_pad, first_kernel)
    first_act = jax.nn.silu(first_pre).astype(jnp.bfloat16)
    act_pad = jnp.pad(first_act, ((2, 0), (1, 1), (0, 0), (0, 0)))
    second_pre = correlate(act_pad, second_kernel)
    critic_map = jax.nn.silu(second_pre).astype(jnp.bfloat16)
    second_delta = (cotangent.astype(jnp.float32) * silu_slope(second_pre)).astype(jnp.bfloat16)
    second_grad = weight_grad(act_pad, second_delta) * grad_scale
    first_back = correlate(jnp.pad(second_delta, ((0, 2), (1, 1), (0, 0), (0, 0))), flipped_kernel(second_kernel))
    first_delta = (first_back * silu_slope(first_pre)).astype(jnp.bfloat16)
    first_grad = weight_grad(clip_pad, first_delta) * grad_scale
    clip_grad = correlate(jnp.pad(first_delta, ((0, 2), (1, 1), (0, 0), (0, 0))), flipped_kernel(first_kernel)).astype(jnp.bfloat16)
    return (critic_map, clip_grad, first_grad, second_grad)
```

```python
import functools

import jax
import jax.numpy as jnp
from jax import lax
from jax.experimental import pallas as pl
from jax.experimental.pallas import tpu as pltpu
from jax.sharding import PartitionSpec as P

MESH = pl.DeviceIdType.MESH
BF16, F32 = jnp.bfloat16, jnp.float32


def silu_slope(value):
    sigma = jax.nn.sigmoid(value)
    return sigma * (1.0 + value * (1.0 - sigma))


def kernel(
    n_frame, n_row, grad_scale,
    clip, w1, w2, cot,
    critic, clip_grad, g1, g2,
    pads, cols0, cols1, cols2, cols3, w1t, w2t, acc, slope1,
    f_send, f_recv, r_send, r_recv,
):
    cols = (cols0, cols1, cols2, cols3)
    _, rows, width, ch = clip.shape
    me_f, me_r = lax.axis_index("frame"), lax.axis_index("row")
    later, earlier = me_f < n_frame - 1, me_f > 0
    below, above = me_r < n_row - 1, me_r > 0
    sides = (
        (later, {"frame": me_f + 1}), (earlier, {"frame": me_f - 1}),
        (below, {"row": me_r + 1}), (above, {"row": me_r - 1}),
    )
    barrier = pltpu.get_barrier_semaphore()
    for there, who in sides:
        @pl.when(there)
        def _():
            pl.semaphore_signal(barrier, inc=1, device_id=who, device_id_type=MESH)

    def zero(ref):
        ref[...] = jnp.zeros(ref.shape, ref.dtype)

    for k in range(4):
        fwd = k < 2

        @pl.when(jnp.logical_not(earlier if fwd else later))
        def _():
            for f in ((0, 1) if fwd else (2, 3)):
                zero(pads.at[k, f])
        local = (2, 3) if fwd else (0, 1)
        halo = (0, 1) if fwd else (2, 3)
        for f in range(4):
            @pl.when(jnp.logical_not(above))
            def _():
                zero(pads.at[k, f, 0])

            @pl.when(jnp.logical_not(below))
            def _():
                zero(pads.at[k, f, rows + 1])
    for t in range(2):
        pads[0, 2 + t, 1 : rows + 1] = clip[t]
    peers = sum(there.astype(jnp.int32) for there, _ in sides)
    pl.semaphore_wait(barrier, peers)

    def frame_copy(k, t):
        fwd = k < 2
        base, hbase = (2, 0) if fwd else (0, 2)
        return pltpu.make_async_remote_copy(
            src_ref=pads.at[k, base + t, pl.ds(1, rows)],
            dst_ref=pads.at[k, hbase + t, pl.ds(1, rows)],
            send_sem=f_send.at[k, t],
            recv_sem=f_recv.at[k, t],
            device_id={"frame": me_f + 1 if fwd else me_f - 1},
            device_id_type=MESH,
        )

    def row_copy(k, f, way):
        src, dst = ((rows, 0), (1, rows + 1))[way]
        return pltpu.make_async_remote_copy(
            src_ref=pads.at[k, f, src],
            dst_ref=pads.at[k, f, dst],
            send_sem=r_send.at[k, f, way],
            recv_sem=r_recv.at[k, f, way],
            device_id={"row": me_r + 1 if way == 0 else me_r - 1},
            device_id_type=MESH,
        )

    def send_rows(k, f):
        @pl.when(below)
        def _():
            row_copy(k, f, 0).start()

        @pl.when(above)
        def _():
            row_copy(k, f, 1).start()

    def wait_rows(k, f):
        @pl.when(above)
        def _():
            row_copy(k, f, 0).wait_recv()

        @pl.when(below)
        def _():
            row_copy(k, f, 1).wait_recv()

    def publish(k, t):
        @pl.when(later if k < 2 else earlier)
        def _():
            frame_copy(k, t).start()
        send_rows(k, (2 if k < 2 else 0) + t)

    def build(k, f):
        def one(r, c):
            x = pads[k, f, r].astype(F32)
            pos = lax.broadcasted_iota(jnp.int32, (width, ch), 0)
            left = jnp.where(pos == 0, 0.0, pltpu.roll(x, 1, 0))
            right = jnp.where(pos == width - 1, 0.0, pltpu.roll(x, width - 1, 0))
            cols[k][f, r, :, 0:ch] = left.astype(BF16)
            cols[k][f, r, :, ch : 2 * ch] = pads[k, f, r]
            cols[k][f, r, :, 2 * ch : 3 * ch] = right.astype(BF16)
            return c
        lax.fori_loop(0, rows + 2, one, 0)

    STEP = 2

    def taps(k, w, t, frames, h, z):
        for a in range(3):
            if t + a not in frames:
                continue
            for b in range(3):
                x = cols[k][t + a, pl.ds(h * STEP + b, STEP)].reshape(STEP * width, 3 * ch)
                d = jnp.dot(x, w[a, b], preferred_element_type=F32)
                z = d if z is None else z + d
        return z

    def stage(k, w, epilogue, between):
        fwd = k < 2
        order = (1, 0) if fwd else (0, 1)
        local, halo = ((2, 3), (0, 1)) if fwd else ((0, 1), (2, 3))
        for t in order:
            wait_rows(k, local[t])
            build(k, local[t])
        for t in order:
            def part(h, c):
                z = taps(k, w, t, local, h, None)
                acc[t, pl.ds(h * STEP, STEP)] = z.reshape(STEP, width, ch)
                return c
            lax.fori_loop(0, rows // STEP, part, 0)
        between()
        for t in order:
            @pl.when(earlier if fwd else later)
            def _():
                frame_copy(k, t).wait_recv()
                send_rows(k, halo[t])
                wait_rows(k, halo[t])
            build(k, halo[t])

            def rest(h, c):
                z = taps(k, w, t, halo, h, acc[t, pl.ds(h * STEP, STEP)].reshape(STEP * width, ch))
                epilogue(t, pl.ds(h * STEP, STEP), h * STEP, z.reshape(STEP, width, ch))
                return c
            lax.fori_loop(0, rows // STEP, rest, 0)
            if k < 3:
                publish(k + 1, t)

    for t in (1, 0):
        publish(0, t)

    def turn_weights():
        def one(i, c):
            a, b = i // 3, lax.rem(i, 3)
            for src, dst in ((w1, w1t), (w2, w2t)):
                for q in range(3):
                    block = src[2 - a, 2 - b, pl.ds((2 - q) * ch, ch), :]
                    dst[a, b, pl.ds(q * ch, ch), :] = block.astype(F32).T.astype(BF16)
            return c
        lax.fori_loop(0, 9, one, 0)

    def weight_grad(kx, kd, out):
        def one(i, c):
            a, b = i // 3, lax.rem(i, 3)
            total = None
            for t in range(2):
                x = cols[kx][t + a, pl.ds(b, rows)].reshape(rows * width, 3 * ch)
                d = pads[kd, t, 1 : rows + 1].reshape(rows * width, ch)
                p = lax.dot_general(x, d, (((0,), (0,)), ((), ())), preferred_element_type=F32)
                total = p if total is None else total + p
            out[a, b] = (total * grad_scale).astype(out.dtype)
            return c
        lax.fori_loop(0, 9, one, 0)

    def end0(t, hs, h, z):
        sigma = jax.nn.sigmoid(z)
        slope1[t, hs] = sigma * (1.0 + z * (1.0 - sigma))
        pads[1, 2 + t, pl.ds(h + 1, STEP)] = (z * sigma).astype(BF16)

    def end1(t, hs, h, z):
        sigma = jax.nn.sigmoid(z)
        critic[t, hs] = (z * sigma).astype(BF16)
        delta = cot[t, hs].astype(F32) * (sigma * (1.0 + z * (1.0 - sigma)))
        pads[2, t, pl.ds(h + 1, STEP)] = delta.astype(BF16)

    def end2(t, hs, h, z):
        pads[3, t, pl.ds(h + 1, STEP)] = (z * slope1[t, hs]).astype(BF16)

    def end3(t, hs, h, z):
        clip_grad[t, hs] = z.astype(BF16)

    stage(0, w1, end0, turn_weights)
    stage(1, w2, end1, lambda: None)
    stage(2, w2t, end2, lambda: weight_grad(1, 2, g2))
    stage(3, w1t, end3, lambda: weight_grad(0, 3, g1))

    for k in range(4):
        fwd = k < 2
        for t in range(2):
            @pl.when(later if fwd else earlier)
            def _():
                frame_copy(k, t).wait_send()
        for f in range(4):
            is_halo = (f < 2) if fwd else (f >= 2)
            has = (earlier if fwd else later) if is_halo else jnp.bool_(True)
            for way, there in ((0, below), (1, above)):
                @pl.when(jnp.logical_and(there, has) if is_halo else there)
                def _():
                    row_copy(k, f, way).wait_send()


def on_device(n_frame, n_row, clip, first_kernel, second_kernel, cotangent):
    frames, rows, width, ch = clip.shape
    grad_scale = 1.0 / float(frames * n_frame * rows * n_row * width) ** 0.5
    vmem = pl.BlockSpec(memory_space=pltpu.VMEM)
    cols = pltpu.VMEM((4, rows + 2, width, 3 * ch), BF16)
    weights = (3, 3, 3 * ch, ch)
    critic, clip_grad, g1, g2 = pl.pallas_call(
        functools.partial(kernel, n_frame, n_row, grad_scale),
        out_shape=(
            jax.ShapeDtypeStruct(clip.shape, BF16),
            jax.ShapeDtypeStruct(clip.shape, BF16),
            jax.ShapeDtypeStruct(weights, BF16),
            jax.ShapeDtypeStruct(weights, BF16),
        ),
        in_specs=[vmem] * 4,
        out_specs=(vmem,) * 4,
        scratch_shapes=[
            pltpu.VMEM((4, 4, rows + 2, width, ch), BF16),
            cols, cols, cols, cols,
            pltpu.VMEM(weights, BF16),
            pltpu.VMEM(weights, BF16),
            pltpu.VMEM(clip.shape, F32),
            pltpu.VMEM(clip.shape, F32),
            pltpu.SemaphoreType.DMA((4, 2)),
            pltpu.SemaphoreType.DMA((4, 2)),
            pltpu.SemaphoreType.DMA((4, 4, 2)),
            pltpu.SemaphoreType.DMA((4, 4, 2)),
        ],
        compiler_params=pltpu.CompilerParams(
            collective_id=0, has_side_effects=True, vmem_limit_bytes=60 * 2**20
        ),
    )(clip, first_kernel.reshape(weights), second_kernel.reshape(weights), cotangent)
    g1, g2 = lax.psum((g1, g2), ("frame", "row"))
    shape = first_kernel.shape
    return critic, clip_grad, g1.astype(F32).reshape(shape), g2.astype(F32).reshape(shape)


def solution(mesh):
    placed = (P("frame", "row", None, None), P(), P(), P("frame", "row", None, None))
    return jax.shard_map(
        functools.partial(on_device, mesh.shape["frame"], mesh.shape["row"]),
        mesh=mesh,
        in_specs=placed,
        out_specs=(P("frame", "row", None, None), P("frame", "row", None, None), P(), P()),
        check_vma=False,
    )
```

```python
import functools

import jax
import jax.numpy as jnp
from jax import lax
from jax.experimental import pallas as pl
from jax.experimental.pallas import tpu as pltpu
from jax.sharding import PartitionSpec as P

MESH = pl.DeviceIdType.MESH
BF16, F32 = jnp.bfloat16, jnp.float32


def silu_slope(value):
    sigma = jax.nn.sigmoid(value)
    return sigma * (1.0 + value * (1.0 - sigma))


def kernel(
    n_frame, n_row, grad_scale,
    clip, w1, w2, cot,
    critic, clip_grad, g1, g2,
    pads, cols0, cols1, cols2, cols3, w1t, w2t, acc, slope1,
    f_send, f_recv, r_send, r_recv,
):
    cols = (cols0, cols1, cols2, cols3)
    _, rows, width, ch = clip.shape
    me_f, me_r = lax.axis_index("frame"), lax.axis_index("row")
    later, earlier = me_f < n_frame - 1, me_f > 0
    below, above = me_r < n_row - 1, me_r > 0
    sides = (
        (later, {"frame": me_f + 1}), (earlier, {"frame": me_f - 1}),
        (below, {"row": me_r + 1}), (above, {"row": me_r - 1}),
    )
    barrier = pltpu.get_barrier_semaphore()
    for there, who in sides:
        @pl.when(there)
        def _():
            pl.semaphore_signal(barrier, inc=1, device_id=who, device_id_type=MESH)

    def zero(ref):
        ref[...] = jnp.zeros(ref.shape, ref.dtype)

    for k in range(4):
        fwd = k < 2

        @pl.when(jnp.logical_not(earlier if fwd else later))
        def _():
            for f in ((0, 1) if fwd else (2, 3)):
                zero(pads.at[k, f])
        local = (2, 3) if fwd else (0, 1)
        halo = (0, 1) if fwd else (2, 3)
        for f in range(4):
            @pl.when(jnp.logical_not(above))
            def _():
                zero(pads.at[k, f, 0])

            @pl.when(jnp.logical_not(below))
            def _():
                zero(pads.at[k, f, rows + 1])
    for t in range(2):
        pads[0, 2 + t, 1 : rows + 1] = clip[t]
    peers = sum(there.astype(jnp.int32) for there, _ in sides)
    pl.semaphore_wait(barrier, peers)

    def frame_copy(k, t):
        fwd = k < 2
        base, hbase = (2, 0) if fwd else (0, 2)
        return pltpu.make_async_remote_copy(
            src_ref=pads.at[k, base + t, pl.ds(1, rows)],
            dst_ref=pads.at[k, hbase + t, pl.ds(1, rows)],
            send_sem=f_send.at[k, t],
            recv_sem=f_recv.at[k, t],
            device_id={"frame": me_f + 1 if fwd else me_f - 1},
            device_id_type=MESH,
        )

    def row_copy(k, f, way):
        src, dst = ((rows, 0), (1, rows + 1))[way]
        return pltpu.make_async_remote_copy(
            src_ref=pads.at[k, f, src],
            dst_ref=pads.at[k, f, dst],
            send_sem=r_send.at[k, f, way],
            recv_sem=r_recv.at[k, f, way],
            device_id={"row": me_r + 1 if way == 0 else me_r - 1},
            device_id_type=MESH,
        )

    def send_rows(k, f):
        @pl.when(below)
        def _():
            row_copy(k, f, 0).start()

        @pl.when(above)
        def _():
            row_copy(k, f, 1).start()

    def wait_rows(k, f):
        @pl.when(above)
        def _():
            row_copy(k, f, 0).wait_recv()

        @pl.when(below)
        def _():
            row_copy(k, f, 1).wait_recv()

    def publish(k, t):
        @pl.when(later if k < 2 else earlier)
        def _():
            frame_copy(k, t).start()
        send_rows(k, (2 if k < 2 else 0) + t)

    def build(k, f):
        def one(r, c):
            x = pads[k, f, r].astype(F32)
            pos = lax.broadcasted_iota(jnp.int32, (width, ch), 0)
            left = jnp.where(pos == 0, 0.0, pltpu.roll(x, 1, 0))
            right = jnp.where(pos == width - 1, 0.0, pltpu.roll(x, width - 1, 0))
            cols[k][f, r, :, 0:ch] = left.astype(BF16)
            cols[k][f, r, :, ch : 2 * ch] = pads[k, f, r]
            cols[k][f, r, :, 2 * ch : 3 * ch] = right.astype(BF16)
            return c
        lax.fori_loop(0, rows + 2, one, 0)

    STEP = 2

    def taps(k, w, t, frames, h, z):
        for a in range(3):
            if t + a not in frames:
                continue
            for b in range(3):
                x = cols[k][t + a, pl.ds(h * STEP + b, STEP)].reshape(STEP * width, 3 * ch)
                d = jnp.dot(x, w[a, b], preferred_element_type=F32)
                z = d if z is None else z + d
        return z

    def stage(k, w, epilogue, between):
        fwd = k < 2
        order = (1, 0) if fwd else (0, 1)
        local, halo = ((2, 3), (0, 1)) if fwd else ((0, 1), (2, 3))
        for t in order:
            wait_rows(k, local[t])
            build(k, local[t])
        for t in order:
            def part(h, c):
                z = taps(k, w, t, local, h, None)
                acc[t, pl.ds(h * STEP, STEP)] = z.reshape(STEP, width, ch)
                return c
            lax.fori_loop(0, rows // STEP, part, 0)
        between()
        for t in order:
            @pl.when(earlier if fwd else later)
            def _():
                frame_copy(k, t).wait_recv()
                send_rows(k, halo[t])
                wait_rows(k, halo[t])
            build(k, halo[t])

            def rest(h, c):
                z = taps(k, w, t, halo, h, acc[t, pl.ds(h * STEP, STEP)].reshape(STEP * width, ch))
                epilogue(t, pl.ds(h * STEP, STEP), h * STEP, z.reshape(STEP, width, ch))
                return c
            lax.fori_loop(0, rows // STEP, rest, 0)
            if k < 3:
                publish(k + 1, t)

    for t in (1, 0):
        publish(0, t)

    def turn_weights():
        def one(i, c):
            a, b = i // 3, lax.rem(i, 3)
            for src, dst in ((w1, w1t), (w2, w2t)):
                for q in range(3):
                    block = src[2 - a, 2 - b, pl.ds((2 - q) * ch, ch), :]
                    dst[a, b, pl.ds(q * ch, ch), :] = block.astype(F32).T.astype(BF16)
            return c
        lax.fori_loop(0, 9, one, 0)

    def weight_grad(kx, kd, out):
        def one(i, c):
            a, b = i // 3, lax.rem(i, 3)
            total = None
            for t in range(2):
                x = cols[kx][t + a, pl.ds(b, rows)].reshape(rows * width, 3 * ch)
                d = pads[kd, t, 1 : rows + 1].reshape(rows * width, ch)
                p = lax.dot_general(x, d, (((0,), (0,)), ((), ())), preferred_element_type=F32)
                total = p if total is None else total + p
            out[a, b] = (total * grad_scale).astype(out.dtype)
            return c
        lax.fori_loop(0, 9, one, 0)

    def end0(t, hs, h, z):
        sigma = jax.nn.sigmoid(z)
        slope1[t, hs] = sigma * (1.0 + z * (1.0 - sigma))
        pads[1, 2 + t, pl.ds(h + 1, STEP)] = (z * sigma).astype(BF16)

    def end1(t, hs, h, z):
        sigma = jax.nn.sigmoid(z)
        critic[t, hs] = (z * sigma).astype(BF16)
        delta = cot[t, hs].astype(F32) * (sigma * (1.0 + z * (1.0 - sigma)))
        pads[2, t, pl.ds(h + 1, STEP)] = delta.astype(BF16)

    def end2(t, hs, h, z):
        pads[3, t, pl.ds(h + 1, STEP)] = (z * slope1[t, hs]).astype(BF16)

    def end3(t, hs, h, z):
        clip_grad[t, hs] = z.astype(BF16)

    stage(0, w1, end0, turn_weights)
    stage(1, w2, end1, lambda: None)
    stage(2, w2t, end2, lambda: weight_grad(1, 2, g2))
    stage(3, w1t, end3, lambda: weight_grad(0, 3, g1))

    for k in range(4):
        fwd = k < 2
        for t in range(2):
            @pl.when(later if fwd else earlier)
            def _():
                frame_copy(k, t).wait_send()
        for f in range(4):
            is_halo = (f < 2) if fwd else (f >= 2)
            has = (earlier if fwd else later) if is_halo else jnp.bool_(True)
            for way, there in ((0, below), (1, above)):
                @pl.when(jnp.logical_and(there, has) if is_halo else there)
                def _():
                    row_copy(k, f, way).wait_send()


def sum_kernel(levels, n, mine, total, buf, landing, s1, q1, s2, q2):
    peers = []
    for axis, step in levels:
        me = lax.axis_index(axis)
        bit = lax.rem(me // step, 2)
        peers.append((bit, {axis: me + (1 - 2 * bit) * step}))
    barrier = pltpu.get_barrier_semaphore()
    for _, who in peers:
        pl.semaphore_signal(barrier, inc=1, device_id=who, device_id_type=MESH)
    pl.semaphore_wait(barrier, len(peers))
    lo, size = 0, n
    for j, (bit, who) in enumerate(peers):
        size //= 2
        keep, give = lo + bit * size, lo + (1 - bit) * size
        src = mine if j == 0 else buf
        copy = pltpu.make_async_remote_copy(
            src_ref=src.at[pl.ds(give, size)],
            dst_ref=landing.at[pl.ds(size, size)],
            send_sem=s1.at[j], recv_sem=q1.at[j],
            device_id=who, device_id_type=MESH,
        )
        copy.start()
        copy.wait()
        last = size == 1

        def add(i, c):
            z = src[keep + i].astype(F32) + landing[size + i].astype(F32)
            dst = total if last else buf
            dst[keep + i] = z.astype(BF16)
            return c
        lax.fori_loop(0, size, add, 0)
        lo = keep
    for j in range(len(peers) - 1, -1, -1):
        bit, who = peers[j]
        copy = pltpu.make_async_remote_copy(
            src_ref=total.at[pl.ds(lo, size)],
            dst_ref=total.at[pl.ds(lo, size)],
            send_sem=s2.at[j], recv_sem=q2.at[j],
            device_id=who, device_id_type=MESH,
        )
        copy.start()
        copy.wait()
        lo, size = lo - bit * size, size * 2


def summed(n_frame, n_row, flat):
    n = n_frame * n_row
    levels = [("row", 1 << b) for b in range(n_row.bit_length() - 1)]
    levels += [("frame", 1 << b) for b in range(n_frame.bit_length() - 1)]
    length, ch = flat.shape
    chunk = -(-length // (16 * n)) * 16
    mine = jnp.pad(flat, ((0, chunk * n - length), (0, 0))).reshape(n, chunk, ch)
    vmem = pl.BlockSpec(memory_space=pltpu.VMEM)
    sems = pltpu.SemaphoreType.DMA((len(levels),))
    out = pl.pallas_call(
        functools.partial(sum_kernel, levels, n),
        out_shape=jax.ShapeDtypeStruct(mine.shape, BF16),
        in_specs=[vmem],
        out_specs=vmem,
        scratch_shapes=[pltpu.VMEM(mine.shape, BF16), pltpu.VMEM(mine.shape, BF16), sems, sems, sems, sems],
        compiler_params=pltpu.CompilerParams(
            collective_id=1, has_side_effects=True, vmem_limit_bytes=32 * 2**20
        ),
    )(mine)
    return out.reshape(n * chunk, ch)[:length]


def on_device(n_frame, n_row, clip, first_kernel, second_kernel, cotangent):
    frames, rows, width, ch = clip.shape
    grad_scale = 1.0 / float(frames * n_frame * rows * n_row * width) ** 0.5
    vmem = pl.BlockSpec(memory_space=pltpu.VMEM)
    cols = pltpu.VMEM((4, rows + 2, width, 3 * ch), BF16)
    weights = (3, 3, 3 * ch, ch)
    critic, clip_grad, g1, g2 = pl.pallas_call(
        functools.partial(kernel, n_frame, n_row, grad_scale),
        out_shape=(
            jax.ShapeDtypeStruct(clip.shape, BF16),
            jax.ShapeDtypeStruct(clip.shape, BF16),
            jax.ShapeDtypeStruct(weights, BF16),
            jax.ShapeDtypeStruct(weights, BF16),
        ),
        in_specs=[vmem] * 4,
        out_specs=(vmem,) * 4,
        scratch_shapes=[
            pltpu.VMEM((4, 4, rows + 2, width, ch), BF16),
            cols, cols, cols, cols,
            pltpu.VMEM(weights, BF16),
            pltpu.VMEM(weights, BF16),
            pltpu.VMEM(clip.shape, F32),
            pltpu.VMEM(clip.shape, F32),
            pltpu.SemaphoreType.DMA((4, 2)),
            pltpu.SemaphoreType.DMA((4, 2)),
            pltpu.SemaphoreType.DMA((4, 4, 2)),
            pltpu.SemaphoreType.DMA((4, 4, 2)),
        ],
        compiler_params=pltpu.CompilerParams(
            collective_id=0, has_side_effects=True, vmem_limit_bytes=60 * 2**20
        ),
    )(clip, first_kernel.reshape(weights), second_kernel.reshape(weights), cotangent)
    shape = first_kernel.shape
    flat = jnp.concatenate([g1.reshape(-1, ch), g2.reshape(-1, ch)])
    both = summed(n_frame, n_row, flat)
    g1, g2 = both[: both.shape[0] // 2], both[both.shape[0] // 2 :]
    return critic, clip_grad, g1.astype(F32).reshape(shape), g2.astype(F32).reshape(shape)


def solution(mesh):
    placed = (P("frame", "row", None, None), P(), P(), P("frame", "row", None, None))
    return jax.shard_map(
        functools.partial(on_device, mesh.shape["frame"], mesh.shape["row"]),
        mesh=mesh,
        in_specs=placed,
        out_specs=(P("frame", "row", None, None), P("frame", "row", None, None), P(), P()),
        check_vma=False,
    )
```
